32 devices in a mesh: bulk: 8 (over z, y), col: 4 (over x, core).
Axes of the slice: x: 2, y: 2, z: 4, core: 2. Of those that a mesh axis runs over, the one named last changes fastest.
Arguments:
- sigma_m: bfloat16 [16384, 16384], P('bulk', 'col'), may hold values from -0.046875 to 0.046875
- sigma_n: bfloat16 [16384, 16384], P('bulk', 'col'), may hold values from -0.046875 to 0.046875
- coeffs: bfloat16 [24576, 16384], P('bulk', 'col'), may hold values from -0.0390625 to 0.0390625
- s_half: bfloat16 [24576, 512], P(('bulk', 'col')), may hold values from -6 to 6
Outputs:
- updated: float32 [24576, 512], P(('bulk', 'col'))
The draws below stay inside these ranges and needn't reach their ends.
All inputs are finite; a program needn't handle non-finite values.
Results may differ from the reference program's by a relative error of at most 0.0051.
Values may be sent and summed in bfloat16 or wider, within the bound.
No kernel may reach another device: no remote copies, remote signals or barrier semaphores. Data moves between devices by JAX's collectives and lax.ppermute only.
A program may use at most 128 MiB of HBM per device.

```python
import jax
import jax.numpy as jnp
from jax import lax

BASIS = 24576
STATES = 16384
PANEL = 512


def block_scale(own_key, dims, split, low, largest):
    factor_of = 1.0
    for axis_at, parts in split:
        heights = jax.random.uniform(jax.random.fold_in(jax.random.fold_in(own_key, 6), axis_at), (parts,), jnp.float32, low / len(split), largest / len(split))
        factor_of = factor_of * jnp.repeat(jnp.exp(heights), dims[axis_at] // parts).reshape((-1,) + (1,) * (len(dims) - 1 - axis_at))
    return factor_of


def noise(key, extent, spread, bound, pieces=(), dtype=jnp.bfloat16):
    result = spread * jax.random.normal(key, extent, jnp.float32)
    if pieces:
        result = result * block_scale(key, extent, pieces, -0.22, 0.18)
    return jnp.clip(result, -bound, bound).astype(dtype)


def setup_inputs(seed: int = 0) -> dict:
    seeds = jax.random.split(jax.random.key(seed), 5)
    sigma_m = noise(seeds[0], (STATES, STATES), STATES ** -0.5, 0.046875, ((0, 8), (1, 4)))
    sigma_n = noise(seeds[1], (STATES, STATES), STATES ** -0.5, 0.046875, ((0, 8), (1, 4)))
    coeffs = noise(seeds[2], (BASIS, STATES), BASIS ** -0.5, 0.0390625, ((0, 8), (1, 4)))
    s_half = noise(seeds[3], (BASIS, PANEL), 1.0, 6.0, ((0, 32),))
    return {"sigma_m": sigma_m, "sigma_n": sigma_n, "coeffs": coeffs, "s_half": s_half}


def reference(sigma_m, sigma_n, coeffs, s_half):
    mixed = (0.5 * (sigma_m.astype(jnp.float32) + sigma_n.astype(jnp.float32))).astype(jnp.bfloat16)
    projected = lax.dot_general(coeffs, s_half, (((0,), (0,)), ((), ())), preferred_element_type=jnp.float32).astype(jnp.bfloat16)
    direct = jnp.dot(mixed, projected, preferred_element_type=jnp.float32)
    flipped = lax.dot_general(mixed, projected, (((0,), (0,)), ((), ())), preferred_element_type=jnp.float32)
    rotated = (0.5 * (direct + flipped)).astype(jnp.bfloat16)
    return jnp.dot(coeffs, rotated, preferred_element_type=jnp.float32)
```

```python
import jax
import jax.numpy as jnp
from jax import lax
from jax.sharding import PartitionSpec as P

AXES = ("bulk", "col")
CHUNKS = 2
F32 = jnp.float32
BF16 = jnp.bfloat16


class Grid:
    def __init__(self, bulk, col):
        self.bulk, self.col = bulk, col
        self.zs, self.xs = bulk // 2, col // 2
        b, c = lax.axis_index("bulk"), lax.axis_index("col")
        self.z, self.y, self.x, self.core = b // 2, b % 2, c // 2, c % 2
        self.per_col = bulk // col
        self.root_col = b // self.per_col
        self.root_core = self.root_col % 2
        self.is_root = self.root_col == c
        self.on_root_core = self.root_core == self.core
        self.sub = b % self.per_col

    def root(self, z, y):
        return divmod((z * 2 + y) // self.per_col, 2)

    def send(self, value, target):
        pairs = []
        for z in range(self.zs):
            for y in range(2):
                for x in range(self.xs):
                    for core in range(2):
                        to = target(z, y, x, core)
                        if to is not None:
                            at = ((z * 2 + y) * self.xs + x) * 2 + core
                            pairs.append((at, ((to[0] * 2 + to[1]) * self.xs + to[2]) * 2 + to[3]))
        return lax.ppermute(value, AXES, pairs)

    def swap_core(self, value):
        return self.send(value, lambda z, y, x, core: (z, y, x, 1 - core))

    def swap_y(self, value):
        return self.send(value, lambda z, y, x, core: (z, 1 - y, x, core))

    def shift_x(self, value, k):
        return self.send(value, lambda z, y, x, core: (z, y, (x + k) % self.xs, core))

    def shift_z(self, value, k):
        return self.send(value, lambda z, y, x, core: ((z + k) % self.zs, y, x, core))


def rows(value, start, size):
    return lax.dynamic_slice_in_dim(value, start, size, 0)


def put(buffer, value, start):
    return lax.dynamic_update_slice_in_dim(buffer, value, start, 0)


def gather_col(g, own):
    n = own.shape[0]
    full = jnp.zeros((g.col * n, own.shape[1]), own.dtype)
    full = put(full, own, (g.x * 2 + g.core) * n)
    far = [(k, g.shift_x(own, k)) for k in range(1, g.xs)]
    full = put(full, g.swap_core(own), (g.x * 2 + 1 - g.core) * n)
    for k, part in far:
        at = (g.x - k) % g.xs * 2
        full = put(full, part, (at + g.core) * n)
        full = put(full, g.swap_core(part), (at + 1 - g.core) * n)
    return full


def scatter_bulk(g, partial, extra):
    half = partial.shape[0] // 2
    part = half // g.zs
    got = g.swap_y(rows(partial, (1 - g.y) * half, half).astype(BF16))

    def summed(z):
        value = rows(partial, g.y * half + z * part, part) + rows(got, z * part, part).astype(F32)
        if extra is not None:
            value = value + rows(extra, z * part, part)
        return value

    order = sorted(range(1, g.zs), key=lambda k: abs(2 * k - g.zs))
    arrived = [g.shift_z(summed((g.z + k) % g.zs).astype(BF16), k) for k in order]
    total = summed(g.z)
    for value in arrived:
        total = total + value.astype(F32)
    return total


def gather_bulk(g, own):
    part = own.shape[0]
    half = part * g.zs
    mine = put(jnp.zeros((half, own.shape[1]), own.dtype), own, g.z * part)
    order = sorted(range(1, g.zs), key=lambda k: abs(2 * k - g.zs))
    for k, value in [(k, g.shift_z(own, k)) for k in order]:
        mine = put(mine, value, (g.z - k) % g.zs * part)
    other = g.swap_y(mine)
    full = put(jnp.zeros((2 * half, own.shape[1]), own.dtype), mine, g.y * half)
    return mine, put(full, other, (1 - g.y) * half)


def spread_rows(g, value):
    def along_x(k):
        def target(z, y, x, core):
            rx, rcore = g.root(z, y)
            return (z, y, (rx + k) % g.xs, core) if (x, core) == (rx, rcore) else None

        return target

    held = jnp.where(g.is_root, value, jnp.zeros_like(value))
    for k in range(1, g.xs):
        held = held + g.send(value, along_x(k))
    got = g.send(held, lambda z, y, x, core: (z, y, x, 1 - core) if core == g.root(z, y)[1] else None)
    return jnp.where(g.on_root_core, held, got)


def sum_rows(g, value):
    value = value + g.send(value, lambda z, y, x, core: (z, y, x, 1 - core) if core != g.root(z, y)[1] else None)

    def along_x(k):
        def target(z, y, x, core):
            rx, rcore = g.root(z, y)
            return (z, y, rx, core) if core == rcore and x == (rx + k) % g.xs else None

        return target

    narrow = value.astype(BF16)
    for k in range(1, g.xs):
        value = value + g.send(narrow, along_x(k)).astype(F32)
    return jnp.where(g.is_root, value, jnp.zeros_like(value))


def scatter_col(g, partial):
    n = partial.shape[0] // g.col
    width = partial.shape[1]
    cut = partial.reshape(g.xs, 2, n, width)
    pair = lax.dynamic_index_in_dim(cut, g.core, 1, False) + g.swap_core(
        lax.dynamic_index_in_dim(cut, 1 - g.core, 1, False)
    )
    total = lax.dynamic_index_in_dim(pair, g.x, 0, False)
    for k in range(1, g.xs):
        piece = lax.dynamic_index_in_dim(pair, (g.x + k) % g.xs, 0, False).astype(BF16)
        total = total + g.shift_x(piece, k).astype(F32)
    return total


def dot(a, b, dim):
    return lax.dot_general(a, b, (((dim,), (0,)), ((), ())), preferred_element_type=F32)


def shards(sigma_m, sigma_n, coeffs, s_half):
    g = Grid(lax.axis_size("bulk"), lax.axis_size("col"))
    width = s_half.shape[1]
    step = width // CHUNKS
    row_states, col_states = sigma_m.shape
    aligned = g.per_col == 2

    mixed = (0.5 * (sigma_m.astype(F32) + sigma_n.astype(F32))).astype(BF16)

    def chunk(s):
        proj = scatter_bulk(g, dot(coeffs, gather_col(g, s), 0), None).astype(BF16)
        half, proj_col = gather_bulk(g, proj)
        own_rows = half if aligned else rows(proj_col, g.sub * row_states, row_states)
        proj_row = spread_rows(g, own_rows)
        row_sum = sum_rows(g, dot(mixed, proj_col, 1))
        col_term = dot(mixed, proj_row, 0)
        if aligned:
            total = scatter_bulk(g, col_term, row_sum)
        else:
            placed = put(jnp.zeros((col_states, step), F32), row_sum, g.sub * row_states)
            total = scatter_bulk(g, col_term + placed, None)
        _, rotated = gather_bulk(g, (0.5 * total).astype(BF16))
        return scatter_col(g, dot(coeffs, rotated, 1))

    return jnp.concatenate([chunk(s_half[:, i * step : (i + 1) * step]) for i in range(CHUNKS)], axis=1)


def solution(mesh):
    return jax.shard_map(
        shards,
        mesh=mesh,
        in_specs=(P("bulk", "col"), P("bulk", "col"), P("bulk", "col"), P(("bulk", "col"), None)),
        out_specs=P(("bulk", "col"), None),
        check_vma=False,
    )
```

```python
import jax
import jax.numpy as jnp
from jax import lax
from jax.experimental.layout import Layout, with_layout_constraint
from jax.sharding import PartitionSpec as P

AXES = ("bulk", "col")
F32 = jnp.float32
BF16 = jnp.bfloat16


class Grid:
    def __init__(self, bulk, col):
        self.bulk, self.col = bulk, col
        self.zs, self.xs = bulk // 2, col // 2
        b, c = lax.axis_index("bulk"), lax.axis_index("col")
        self.z, self.y, self.x, self.core = b // 2, b % 2, c // 2, c % 2
        self.per_col = bulk // col
        self.root_col = b // self.per_col
        self.root_core = self.root_col % 2
        self.is_root = self.root_col == c
        self.on_root_core = self.root_core == self.core
        self.sub = b % self.per_col

    def root(self, z, y):
        return divmod((z * 2 + y) // self.per_col, 2)

    def send(self, value, target):
        pairs = []
        for z in range(self.zs):
            for y in range(2):
                for x in range(self.xs):
                    for core in range(2):
                        to = target(z, y, x, core)
                        if to is not None:
                            at = ((z * 2 + y) * self.xs + x) * 2 + core
                            pairs.append((at, ((to[0] * 2 + to[1]) * self.xs + to[2]) * 2 + to[3]))
        return lax.ppermute(value, AXES, pairs)

    def swap_core(self, value):
        return self.send(value, lambda z, y, x, core: (z, y, x, 1 - core))

    def swap_y(self, value):
        return self.send(value, lambda z, y, x, core: (z, 1 - y, x, core))

    def shift_x(self, value, k):
        return self.send(value, lambda z, y, x, core: (z, y, (x + k) % self.xs, core))

    def shift_z(self, value, k):
        return self.send(value, lambda z, y, x, core: ((z + k) % self.zs, y, x, core))


def rows(value, start, size):
    return lax.dynamic_slice_in_dim(value, start, size, 0)


def put(buffer, value, start):
    return lax.dynamic_update_slice_in_dim(buffer, value, start, 0)


def after(value, *done):
    return lax.optimization_barrier((value, *done))[0]


def dot(a, b, dim):
    return lax.dot_general(a, b, (((dim,), (0,)), ((), ())), preferred_element_type=F32)


def far_first(n):
    return sorted(range(1, n), key=lambda k: abs(2 * k - n))


def to_z(g, near, got, extra=None):
    part = near.shape[0] // g.zs

    def summed(z):
        value = rows(near, z * part, part) + rows(got, z * part, part).astype(F32)
        return value if extra is None else value + rows(extra, z * part, part)

    return [summed((g.z + k) % g.zs).astype(BF16) for k in far_first(g.zs)], summed(g.z)


def scatter_z(g, pieces, total):
    for piece, k in zip(pieces, far_first(g.zs)):
        total = total + g.shift_z(piece, k).astype(F32)
    return total


def gather_z(g, own):
    part = own.shape[0]
    mine = put(jnp.zeros((part * g.zs, own.shape[1]), own.dtype), own, g.z * part)
    for k, value in [(k, g.shift_z(own, k)) for k in far_first(g.zs)]:
        mine = put(mine, value, (g.z - k) % g.zs * part)
    return mine


def spread_rows(g, value):
    def along_x(k):
        def target(z, y, x, core):
            rx, rcore = g.root(z, y)
            return (z, y, (rx + k) % g.xs, core) if (x, core) == (rx, rcore) else None

        return target

    got = [g.send(value, along_x(k)) for k in range(1, g.xs)]
    held = jnp.where(g.is_root, value, jnp.zeros_like(value))
    for part in got:
        held = held + part
    got = g.send(held, lambda z, y, x, core: (z, y, x, 1 - core) if core == g.root(z, y)[1] else None)
    return jnp.where(g.on_root_core, held, got)


def sum_rows(g, value):
    near = g.send(value.astype(BF16), lambda z, y, x, core: (z, y, x, 1 - core) if core != g.root(z, y)[1] else None)
    value = value + near.astype(F32)

    def along_x(k):
        def target(z, y, x, core):
            rx, rcore = g.root(z, y)
            return (z, y, rx, core) if core == rcore and x == (rx + k) % g.xs else None

        return target

    narrow = value.astype(BF16)
    for k in range(1, g.xs):
        value = value + g.send(narrow, along_x(k)).astype(F32)
    return jnp.where(g.is_root, value, jnp.zeros_like(value))


def both(g, mine, other):
    half = mine.shape[0]
    full = put(jnp.zeros((2 * half, mine.shape[1]), mine.dtype), mine, g.y * half)
    return put(full, other, (1 - g.y) * half)


def join(*values):
    return lax.optimization_barrier(values)


def row_major(value):
    return with_layout_constraint(value, Layout(major_to_minor=tuple(range(value.ndim))))


def shards(sigma_m, sigma_n, coeffs, s_half):
    g = Grid(lax.axis_size("bulk"), lax.axis_size("col"))
    width = s_half.shape[1] // 2
    row_states, col_states = sigma_m.shape
    half = col_states // 2
    n = coeffs.shape[0] // g.col
    aligned = g.per_col == 2
    mine_at, other_at = g.y * half, (1 - g.y) * half
    mixed = (0.5 * (sigma_m.astype(F32) + sigma_n.astype(F32))).astype(BF16)

    def cols(a, at):
        return lax.dynamic_slice_in_dim(a, at, half, 1)

    def send_x(own):
        return [(k, g.shift_x(own, k)) for k in range(1, g.xs)]

    def pair(own, near):
        return jnp.where(g.core == 0, jnp.concatenate([own, near]), jnp.concatenate([near, own]))

    def gathered(own, near, far):
        parts = [(g.x, pair(own, near))]
        for k, value in far:
            parts.append(((g.x - k) % g.xs, pair(value, g.swap_core(value))))
        return parts

    def in_order(parts):
        full = jnp.zeros((g.col * n, width), BF16)
        for x, part in parts:
            full = put(full, part, x * 2 * n)
        return full

    def project(s, at):
        if not isinstance(s, list):
            return dot(cols(coeffs, at), s, 0)
        total = None
        for x, part in s:
            value = dot(lax.dynamic_slice(coeffs, (x * 2 * n, at), (2 * n, half)), part, 0)
            total = value if total is None else total + value
        return total

    def by_rows(mine, other):
        own = mine if aligned else rows(both(g, mine, other), g.sub * row_states, row_states)
        own = spread_rows(g, own)
        far = dot(cols(mixed, other_at), own, 0)
        far = far.astype(BF16) if aligned else far
        return far, dot(cols(mixed, mine_at), own, 0)

    def begin_cols(mine):
        return dot(cols(mixed, mine_at), mine, 1)

    def by_cols(begun, other):
        value = begun + dot(cols(mixed, other_at), other, 1)
        return sum_rows(g, value)

    def merge(far, near, row_sum):
        if aligned:
            return far, near, row_sum
        placed = put(jnp.zeros((col_states, width), F32), row_sum, g.sub * row_states)
        return (far + rows(placed, other_at, half)).astype(BF16), near + rows(placed, mine_at, half), None

    def rotate(mine):
        return row_major(dot(cols(coeffs, mine_at), mine, 1))

    def rotate_rest(other, begun):
        value = row_major(begun + dot(cols(coeffs, other_at), other, 1))
        value = value.reshape(g.xs, 2, n, width)
        theirs = g.swap_core(lax.dynamic_index_in_dim(value, 1 - g.core, 1, False))
        value = lax.dynamic_index_in_dim(value, g.core, 1, False)

        def block(k):
            x = (g.x + k) % g.xs
            return lax.dynamic_index_in_dim(value, x, 0, False) + lax.dynamic_index_in_dim(theirs, x, 0, False)

        got = [g.shift_x(block(k).astype(BF16), k) for k in range(1, g.xs)]
        total = block(0)
        for part in got:
            total = total + part.astype(F32)
        return total

    def along_y(value):
        return g.swap_y(value)

    def sum_z(pieces, total):
        return scatter_z(g, pieces, total)

    def all_z(own):
        return gather_z(g, own)

    s_a, s_b = s_half[:, :width], s_half[:, width:]
    x_a = send_x(s_a)
    c_a = g.swap_core(s_a)
    s_b = after(s_b, *[v for _, v in x_a])
    x_b = send_x(s_b)
    c_b = g.swap_core(s_b)
    parts = gathered(s_a, c_a, x_a)
    far_a = project(parts, other_at).astype(BF16)

    y_a = along_y(far_a)
    near_a = project(in_order(parts), mine_at)
    full_b = in_order(gathered(s_b, c_b, x_b))
    far_b = project(full_b, other_at).astype(BF16)
    send_a, own_a = to_z(g, near_a, y_a)
    *send_a, far_b = join(*send_a, far_b)

    y_b = along_y(far_b)
    near_b = project(full_b, mine_at)
    proj_a = sum_z(send_a, own_a).astype(BF16)
    proj_a, y_b, mixed = join(proj_a, y_b, mixed)

    mine_a = all_z(proj_a)
    send_b, own_b = to_z(g, near_b, y_b)
    mine_a, *send_b = join(mine_a, *send_b)

    other_a = along_y(mine_a)
    proj_b = sum_z(send_b, own_b).astype(BF16)
    begun_a = begin_cols(mine_a)
    far_a, near_a = by_rows(mine_a, other_a)
    far_a, other_a, proj_b, begun_a = join(far_a, other_a, proj_b, begun_a)

    far_a, near_a, sum_a = merge(far_a, near_a, by_cols(begun_a, other_a))
    y_a = along_y(far_a)
    mine_b = all_z(proj_b)
    send_a, own_a = to_z(g, near_a, y_a, sum_a)
    mine_b, *send_a = join(mine_b, *send_a)

    other_b = along_y(mine_b)
    rot_a = (0.5 * sum_z(send_a, own_a)).astype(BF16)
    begun_b = begin_cols(mine_b)
    far_b, near_b = by_rows(mine_b, other_b)
    far_b, other_b, rot_a, begun_b = join(far_b, other_b, rot_a, begun_b)

    far_b, near_b, sum_b = merge(far_b, near_b, by_cols(begun_b, other_b))
    y_b = along_y(far_b)
    mine_a = all_z(rot_a)
    send_b, own_b = to_z(g, near_b, y_b, sum_b)
    mine_a, *send_b = join(mine_a, *send_b)

    other_a = along_y(mine_a)
    rot_b = (0.5 * sum_z(send_b, own_b)).astype(BF16)
    begun_a = rotate(mine_a)
    rot_b, other_a, begun_a = join(rot_b, other_a, begun_a)

    mine_b = all_z(rot_b)
    out_a = rotate_rest(other_a, begun_a)
    other_b = along_y(mine_b)
    begun_b = rotate(mine_b)
    other_b, begun_b, out_a = join(other_b, begun_b, out_a)
    out_b = rotate_rest(other_b, begun_b)
    return jnp.concatenate([out_a, out_b], axis=1)


def solution(mesh):
    return jax.shard_map(
        shards,
        mesh=mesh,
        in_specs=(P("bulk", "col"), P("bulk", "col"), P("bulk", "col"), P(("bulk", "col"), None)),
        out_specs=P(("bulk", "col"), None),
        check_vma=False,
    )
```
